128 devices in a mesh: seq: 64 (over x, y, z), head: 2 (over core).
Axes of the slice: x: 4, y: 4, z: 4, core: 2. Of those that a mesh axis runs over, the one named last changes fastest.
Arguments:
- tokens: bfloat16 [65536, 2048], P('seq'), may hold values from -6 to 6
- w_query: bfloat16 [2048, 256], P(None, 'head'), may hold values from -0.25 to 0.25
- w_key: bfloat16 [2048, 256], P(None, 'head'), may hold values from -0.25 to 0.25
- w_value: bfloat16 [2048, 2048], P(None, 'head'), may hold values from -0.125 to 0.125
- w_out: bfloat16 [2048, 2048], replicated, may hold values from -1.796875 to 1.796875
Outputs:
- mixed: bfloat16 [65536, 2048], P('seq', 'head')
The draws below stay inside these ranges and needn't reach their ends.
All inputs are finite; a program needn't handle non-finite values.
Results may differ from the reference program's by a relative error of at most 0.011.
Values may be sent and summed in bfloat16 or wider, within the bound.
A program may use at most 128 MiB of HBM per device.

```python
import jax
import jax.numpy as jnp
from jax import lax

D = 2048
HEADS = 16
KEY_DIM = 16
VALUE_DIM = 128
TOK_DEV = 1024
FEATURES = 273
TOKENS = 65536
N_SEQ = 64


def steps_of(stream_key, extent, split, least, largest):
    factor_of, own = 1.0, jax.random.fold_in(stream_key, 6)
    for axis_at, shards_of in split:
        draws = jnp.exp(jax.random.uniform(jax.random.fold_in(own, axis_at), (shards_of,), jnp.float32, least / len(split), largest / len(split)))
        factor_of = factor_of * jnp.repeat(draws, extent[axis_at] // shards_of).reshape([-1 if axis == axis_at else 1 for axis in range(len(extent))])
    return factor_of


def normal_values(own_key, dims, spread, most, split=(), held_as=jnp.bfloat16):
    result = spread * jax.random.normal(own_key, dims, jnp.float32)
    if split:
        result = result * steps_of(own_key, dims, split, -0.22, 0.18)
    return jnp.clip(result, -most, most).astype(held_as)


def setup_inputs(seed: int = 0) -> dict:
    seeds = jax.random.split(jax.random.key(seed), 6)
    tokens = normal_values(seeds[0], (TOKENS, D), 1.0, 6.0, ((0, 64),))
    w_query = normal_values(seeds[1], (D, HEADS * KEY_DIM), (D // 4) ** -0.5, 0.25, ((1, 2),))
    w_key = normal_values(seeds[2], (D, HEADS * KEY_DIM), (D // 4) ** -0.5, 0.25, ((1, 2),))
    w_value = normal_values(seeds[3], (D, HEADS * VALUE_DIM), D ** -0.5, 0.125, ((1, 2),))
    w_out = normal_values(seeds[4], (HEADS * VALUE_DIM, D), 0.3, 1.796875)
    return dict(tokens=tokens, w_query=w_query, w_key=w_key, w_value=w_value, w_out=w_out)


def taylor_features(rows):
    wide = rows.astype(jnp.float32)
    count = wide.shape[-1]
    outer = (wide[..., :, None] * wide[..., None, :]).reshape(wide.shape[:-1] + (count * count,))
    ones = jnp.ones(wide.shape[:-1] + (1,), jnp.float32)
    joined = jnp.concatenate([ones, wide / (count ** 0.25), outer / ((2.0 * count) ** 0.5)], axis=-1)
    return joined.astype(jnp.bfloat16)


def reference(tokens, w_query, w_key, w_value, w_out):
    def span_step(carry, span_rows):
        prefix, zprefix = carry
        queries = jnp.dot(span_rows, w_query, preferred_element_type=jnp.float32).astype(jnp.bfloat16).reshape(TOK_DEV, HEADS, KEY_DIM)
        key_rows = jnp.dot(span_rows, w_key, preferred_element_type=jnp.float32).astype(jnp.bfloat16).reshape(TOK_DEV, HEADS, KEY_DIM)
        val_rows = jnp.dot(span_rows, w_value, preferred_element_type=jnp.float32).astype(jnp.bfloat16).reshape(TOK_DEV, HEADS, VALUE_DIM)
        query_feat = taylor_features(queries)
        key_feat = taylor_features(key_rows)
        state = jnp.einsum('thf,thv->hfv', key_feat.astype(jnp.float32), val_rows.astype(jnp.float32), precision=lax.Precision.HIGHEST)
        norm_sum = jnp.sum(key_feat.astype(jnp.float32), axis=0)
        prefix_low = prefix.astype(jnp.bfloat16)
        numer_pre = jnp.einsum('thf,hfv->thv', query_feat.astype(jnp.float32), prefix_low.astype(jnp.float32), precision=lax.Precision.HIGHEST)
        denom_pre = jnp.einsum('thf,hf->th', query_feat.astype(jnp.float32), zprefix, precision=lax.Precision.HIGHEST)
        block = min(512, TOK_DEV)
        outputs = []
        for index in range(TOK_DEV // block):
            low = index * block
            high = low + block
            q_block = queries[low:high].astype(jnp.float32)
            k_block = key_rows[:high].astype(jnp.float32)
            scores = jnp.einsum('qhd,khd->hqk', q_block, k_block) / (KEY_DIM ** 0.5)
            taylor = 1.0 + scores + 0.5 * scores * scores
            row_ids = low + jnp.arange(block, dtype=jnp.int32)[:, None]
            col_ids = jnp.arange(high, dtype=jnp.int32)[None, :]
            taylor = jnp.where((col_ids <= row_ids)[None], taylor, 0.0)
            denom = denom_pre[low:high] + jnp.transpose(jnp.sum(taylor, axis=-1))
            taylor_low = taylor.astype(jnp.bfloat16)
            numer_in = jnp.einsum('hqk,khv->qhv', taylor_low.astype(jnp.float32), val_rows[:high].astype(jnp.float32))
            numer = numer_pre[low:high] + numer_in
            outputs.append((numer / denom[..., None]).astype(jnp.bfloat16))
        attended = jnp.concatenate(outputs, axis=0).reshape(TOK_DEV, HEADS * VALUE_DIM)
        mixed_rows = jnp.dot(attended, w_out, preferred_element_type=jnp.float32).astype(jnp.bfloat16)
        return (prefix + state, zprefix + norm_sum), mixed_rows

    init = (jnp.zeros((HEADS, FEATURES, VALUE_DIM), jnp.float32), jnp.zeros((HEADS, FEATURES), jnp.float32))
    spans = tokens.reshape(N_SEQ, TOK_DEV, D)
    final, mixed = lax.scan(span_step, init, spans)
    return mixed.reshape(TOKENS, D)
```

```python
import jax
import jax.numpy as jnp
from jax import lax
from jax.experimental import pallas as pl
from jax.experimental.pallas import tpu as pltpu
from jax.sharding import PartitionSpec as P

TOK = 1024
D = 2048
HERE = 8
CHUNK = 256
NCH = TOK // CHUNK
FEAT = 160
HALF = FEAT // 2
PLANE = 16
XN = 4
MESH = pl.DeviceIdType.MESH
C2 = 1.0 / (32.0**0.5)
BF = jnp.bfloat16
F32 = jnp.float32


def dot(a, b):
    return jnp.dot(a, b, preferred_element_type=F32)


def iota(shape, dim):
    return lax.broadcasted_iota(jnp.int32, shape, dim)


def kernel(
    tok_hbm, wq_hbm, wk_hbm, wv_hbm, wo_hbm, out_hbm,
    tok, wqk, wv, wo, q_s, kt, ktb, v_s, phiq, pk, ea, eb, lext, numer,
    sbuf, rbuf, xs, xbuf, obuf, pbuf, att, outv,
    tok_sem, wqk_sem, wv_sem, wo_sem, out_sem,
    s_send, s_recv, x_send, x_recv, p_send, p_recv, a_send, a_recv,
):
    seq = lax.axis_index("seq")
    core = lax.axis_index("head")
    xp = seq // PLANE
    me = lax.rem(seq, PLANE)

    def wqk_copy(j):
        src = (wq_hbm, wk_hbm)[j]
        return pltpu.make_async_copy(src, wqk.at[:, pl.ds(j * 128, 128)], wqk_sem.at[j])

    def tok_copy(b):
        rows = pl.ds(b * CHUNK, CHUNK)
        return pltpu.make_async_copy(tok_hbm.at[rows, :], tok.at[rows, :], tok_sem.at[b])

    def wv_copy(j):
        cols = pl.ds(pl.multiple_of(j * 256, 256), 256)
        return pltpu.make_async_copy(wv_hbm.at[:, cols], wv.at[j], wv_sem.at[j])

    def wo_copy(j):
        cols = pl.ds(pl.multiple_of(core * 1024 + j * 256, 256), 256)
        return pltpu.make_async_copy(wo_hbm.at[:, cols], wo.at[j], wo_sem.at[j])

    for j in range(2):
        wqk_copy(j).start()
    for b in range(NCH):
        tok_copy(b).start()
    for j in range(4):
        wv_copy(j).start()
    for j in range(4):
        wo_copy(j).start()

    barrier = pltpu.get_barrier_semaphore()

    def greet(i, c):
        @pl.when(i != me)
        def _():
            pl.semaphore_signal(
                barrier, inc=1, device_id={"seq": xp * PLANE + i}, device_id_type=MESH
            )

        return c

    lax.fori_loop(0, PLANE, greet, 0)
    for dx in range(1, XN):
        pl.semaphore_signal(
            barrier,
            inc=1,
            device_id={"seq": lax.rem(xp + dx, XN) * PLANE + me},
            device_id_type=MESH,
        )
    pl.semaphore_signal(barrier, inc=1, device_id={"head": 1 - core}, device_id_type=MESH)

    row = iota((256, 256), 0)
    col = iota((256, 256), 1)
    lane_i = col & 15
    lane_d = (col >> 4) - 1
    ea[...] = jnp.where((row == 128 + lane_i) & (col < 152), 1.0, 0.0).astype(BF)
    eb[...] = jnp.where(
        (row == 128 + ((lane_i + lane_d) & 15)) & (col >= 16) & (col < 152), 1.0, 0.0
    ).astype(BF)

    for j in range(2):
        wqk_copy(j).wait()
    for b in range(NCH):
        tok_copy(b).wait()
        rows = slice(b * CHUNK, (b + 1) * CHUNK)
        qk = dot(tok[rows, :], wqk[...])
        q_s[rows, :] = qk[:, :128].astype(BF)
        k_t = qk[:, 128:].astype(BF).astype(F32).T
        kt[:, rows] = k_t
        ktb[:, rows] = k_t.astype(BF)

    pl.semaphore_wait(barrier, PLANE - 1 + XN - 1 + 1)

    eye = iota((128, 128), 0) == iota((128, 128), 1)
    ones = jnp.ones((CHUNK, 128), BF)
    row16 = iota((16, 128), 0)
    row16w = iota((16, TOK), 0)

    def state_copy(o):
        return pltpu.make_async_remote_copy(
            src_ref=sbuf.at[o], dst_ref=rbuf.at[me], send_sem=s_send.at[o],
            recv_sem=s_recv.at[me], device_id={"seq": xp * PLANE + o}, device_id_type=MESH,
        )

    def state_arrival(q):
        return pltpu.make_async_remote_copy(
            src_ref=sbuf.at[q], dst_ref=rbuf.at[q], send_sem=s_send.at[q],
            recv_sem=s_recv.at[q], device_id={"seq": xp * PLANE + q}, device_id_type=MESH,
        )

    def total_copy(dx):
        return pltpu.make_async_remote_copy(
            src_ref=xs, dst_ref=xbuf.at[xp], send_sem=x_send.at[dx - 1], recv_sem=x_recv.at[xp],
            device_id={"seq": lax.rem(xp + dx, XN) * PLANE + me}, device_id_type=MESH,
        )

    def total_arrival(dx):
        other = lax.rem(xp + dx, XN)
        return pltpu.make_async_remote_copy(
            src_ref=xs, dst_ref=xbuf.at[other], send_sem=x_send.at[dx - 1],
            recv_sem=x_recv.at[other], device_id={"seq": other * PLANE + me}, device_id_type=MESH,
        )

    def prefix_copy(q):
        return pltpu.make_async_remote_copy(
            src_ref=obuf.at[q], dst_ref=pbuf.at[me], send_sem=p_send.at[q],
            recv_sem=p_recv.at[me], device_id={"seq": xp * PLANE + q}, device_id_type=MESH,
        )

    def prefix_arrival(o):
        return pltpu.make_async_remote_copy(
            src_ref=obuf.at[o], dst_ref=pbuf.at[o], send_sem=p_send.at[o],
            recv_sem=p_recv.at[o], device_id={"seq": xp * PLANE + o}, device_id_type=MESH,
        )

    def att_copy(h, side):
        cols = pl.ds(pl.multiple_of((side * HERE + h) * 128, 128), 128)
        return pltpu.make_async_remote_copy(
            src_ref=att.at[:, cols], dst_ref=att.at[:, cols], send_sem=a_send.at[h],
            recv_sem=a_recv.at[h], device_id={"head": 1 - core}, device_id_type=MESH,
        )

    def pair(hp, c):
        wv_copy(hp).wait()
        v_s[hp] = dot(tok[...], wv[hp]).astype(BF)
        for j in range(2):
            h = 2 * hp + j
            u = kt[pl.ds(pl.multiple_of(h * 16, 16), 16), :]
            pk[j, 0:16, :] = (u * 0.5).astype(BF)
            for d in range(8):
                other = u if d == 0 else pltpu.roll(u, 16 - d, 0)
                pk[j, 16 + 16 * d : 32 + 16 * d, :] = (u * other * C2).astype(BF)
            last = u * pltpu.roll(u, 8, 0) * C2
            last = jnp.where(row16w < 8, last, jnp.where(row16w == 8, 1.0, 0.0))
            pk[j, 144:160, :] = last.astype(BF)
        for j in range(2):
            h = 2 * hp + j
            run = None
            for b in range(NCH):
                rows = slice(b * CHUNK, (b + 1) * CHUNK)
                vals = jnp.concatenate([v_s[hp, rows, j * 128 : (j + 1) * 128], ones], axis=1)
                part = dot(pk[j, :, rows], vals)
                run = part if run is None else run + part
                if b < NCH - 1:
                    lext[h, b] = run.astype(BF)
            zc = run[:, 128:]
            z0 = jnp.sum(jnp.where(eye, zc[:128], 0.0), axis=0, keepdims=True)
            z1 = jnp.sum(jnp.where(eye[:32], zc[128:], 0.0), axis=0, keepdims=True)
            tail = jnp.where(row16 == 14, z0, jnp.where(row16 == 15, z1, run[144:160, :128]))
            sbuf[2 * h] = run[:HALF, :128].astype(BF)
            sbuf[2 * h + 1, 0:64, :] = run[HALF:144, :128].astype(BF)
            sbuf[2 * h + 1, 64:80, :] = tail.astype(BF)
        for j in range(4):
            o = 4 * hp + j

            @pl.when(o != me)
            def _():
                state_copy(o).start()

            @pl.when(o == me)
            def _():
                rbuf[me] = sbuf[o]

        return c

    lax.fori_loop(0, 4, pair, 0)

    lane = iota((1, 256), 1)
    c1 = jnp.where(lane < 16, 1.0, 0.0)
    c0 = jnp.where(lane == 152, 2.0, 0.0)
    scale = jnp.where(lane < 16, 1.0, jnp.where(lane < 32, 2.0 * C2, 4.0 * C2))
    lane128 = iota((1, 128), 1)
    causal = iota((CHUNK, CHUNK), 1) <= iota((CHUNK, CHUNK), 0)

    def inside(h, c):
        low = pl.multiple_of(128 - 16 * h, 16)
        ea_h = ea[pl.ds(low, 128), :]
        eb_h = eb[pl.ds(low, 128), :]
        own = jnp.where((lane128 >> 4) == h, 0.25, 0.0).astype(BF)
        hp = h // 2
        vcols = pl.ds(pl.multiple_of(lax.rem(h, 2) * 128, 128), 128)
        for b in range(NCH):
            rows = slice(b * CHUNK, (b + 1) * CHUNK)
            qb = q_s[rows, :]
            first = dot(qb, ea_h)
            second = dot(qb, eb_h)
            feat = (first * (second + c1) * scale + c0).astype(BF)
            phiq[h, rows, :] = feat
            t = dot(qb * own, ktb[:, rows]) + 1.0
            t = jnp.where(causal, t * t + 1.0, 0.0).astype(BF)
            vals = jnp.concatenate([v_s[hp, rows, vcols], ones], axis=1)
            r = dot(t, vals)
            if b > 0:
                r = r + dot(feat[:, :FEAT], lext[h, b - 1])
            numer[h, rows, :] = r
        return c

    def owner_reduce():
        def arrive(q, c):
            @pl.when(q != me)
            def _():
                state_arrival(q).wait_recv()

            return c

        lax.fori_loop(0, PLANE, arrive, 0)
        tot = lax.fori_loop(
            0, PLANE, lambda q, a: a + rbuf[q].astype(F32), jnp.zeros((HALF, 128), F32)
        )
        xs[...] = tot.astype(BF)
        for dx in range(1, XN):
            total_copy(dx).start()

    def owner_prefix():
        for dx in range(1, XN):
            total_arrival(dx).wait_recv()
        base = lax.fori_loop(
            0, xp, lambda k, a: a + xbuf[k].astype(F32), jnp.zeros((HALF, 128), F32)
        )

        def step(q, a):
            obuf[q] = a.astype(BF)
            return a + rbuf[q].astype(F32)

        lax.fori_loop(0, PLANE, step, base)

        def give(q, c):
            @pl.when(q != me)
            def _():
                prefix_copy(q).start()

            @pl.when(q == me)
            def _():
                pbuf[me] = obuf[q]

            return c

        lax.fori_loop(0, PLANE, give, 0)

    lax.fori_loop(0, 4, inside, 0)
    owner_reduce()
    lax.fori_loop(4, 6, inside, 0)
    owner_prefix()
    lax.fori_loop(6, 8, inside, 0)

    ones128 = jnp.ones((128, 128), BF)

    def finish(h, c):
        for j in range(2):
            o = 2 * h + j

            @pl.when(o != me)
            def _():
                prefix_arrival(o).wait_recv()

        top = pbuf[2 * h]
        bottom = pbuf[2 * h + 1]
        zz = bottom[64:80].astype(F32)
        m0 = jnp.where(eye, zz[14:15], 0.0).astype(BF)
        m1 = jnp.where(eye[:32], zz[15:16], 0.0).astype(BF)
        zb = dot(jnp.concatenate([m0, m1], axis=0), ones128).astype(BF)
        pre = jnp.concatenate([jnp.concatenate([top, bottom], axis=0), zb], axis=1)
        cols = pl.ds(pl.multiple_of((core * HERE + h) * 128, 128), 128)
        for b in range(NCH):
            rows = slice(b * CHUNK, (b + 1) * CHUNK)
            r = dot(phiq[h, rows, :FEAT], pre) + numer[h, rows, :]
            att[rows, cols] = (r[:, :128] / r[:, 128:]).astype(BF)
        att_copy(h, core).start()
        return c

    lax.fori_loop(0, HERE, finish, 0)

    for h in range(HERE):
        att_copy(h, 1 - core).wait_recv()

    def out_copy(j):
        cols = pl.ds(pl.multiple_of(j * 256, 256), 256)
        return pltpu.make_async_copy(outv.at[j], out_hbm.at[:, cols], out_sem.at[j])

    def project(j, c):
        wo_copy(j).wait()
        outv[j] = dot(att[...], wo[j]).astype(BF)
        out_copy(j).start()
        return c

    lax.fori_loop(0, 4, project, 0)

    def drain(q, c):
        @pl.when(q != me)
        def _():
            state_copy(q).wait_send()
            prefix_copy(q).wait_send()

        return c

    lax.fori_loop(0, PLANE, drain, 0)
    for dx in range(1, XN):
        total_copy(dx).wait_send()
    for h in range(HERE):
        att_copy(h, core).wait_send()
    for j in range(4):
        out_copy(j).wait()


def per_device(tokens, w_query, w_key, w_value, w_out):
    vmem = pltpu.VMEM
    dma = pltpu.SemaphoreType.DMA
    hbm = pl.BlockSpec(memory_space=pl.ANY)
    return pl.pallas_call(
        kernel,
        out_shape=jax.ShapeDtypeStruct((TOK, 1024), BF),
        in_specs=[hbm] * 5,
        out_specs=hbm,
        scratch_shapes=[
            vmem((TOK, D), BF),
            vmem((D, 256), BF),
            vmem((4, D, 256), BF),
            vmem((4, D, 256), BF),
            vmem((TOK, 128), BF),
            vmem((128, TOK), F32),
            vmem((128, TOK), BF),
            vmem((4, TOK, 256), BF),
            vmem((HERE, TOK, 256), BF),
            vmem((2, FEAT, TOK), BF),
            vmem((256, 256), BF),
            vmem((256, 256), BF),
            vmem((HERE, NCH - 1, FEAT, 256), BF),
            vmem((HERE, TOK, 256), F32),
            vmem((PLANE, HALF, 128), BF),
            vmem((PLANE, HALF, 128), BF),
            vmem((HALF, 128), BF),
            vmem((XN, HALF, 128), BF),
            vmem((PLANE, HALF, 128), BF),
            vmem((PLANE, HALF, 128), BF),
            vmem((TOK, D), BF),
            vmem((4, TOK, 256), BF),
            dma((NCH,)), dma((2,)), dma((4,)), dma((4,)), dma((4,)),
            dma((PLANE,)), dma((PLANE,)), dma((XN,)), dma((XN,)),
            dma((PLANE,)), dma((PLANE,)), dma((HERE,)), dma((HERE,)),
        ],
        compiler_params=pltpu.CompilerParams(
            collective_id=0, has_side_effects=True, vmem_limit_bytes=60 * 1024 * 1024
        ),
    )(tokens, w_query, w_key, w_value, w_out)


def solution(mesh):
    in_specs = (P("seq", None), P(None, "head"), P(None, "head"), P(None, "head"), P())
    return jax.shard_map(
        per_device, mesh=mesh, in_specs=in_specs, out_specs=P("seq", "head"), check_vma=False
    )
```

```python
import jax
import jax.numpy as jnp
from jax import lax
from jax.experimental import pallas as pl
from jax.experimental.pallas import tpu as pltpu
from jax.sharding import PartitionSpec as P

TOK = 1024
D = 2048
HERE = 8
CHUNK = 256
NCH = TOK // CHUNK
FEAT = 160
PIECE = FEAT // 4
PLANE = 16
XN = 4
SHIFTS = sorted(
    [(dy, dz) for dy in range(4) for dz in range(4) if dy or dz],
    key=lambda s: -(min(s[0], 4 - s[0]) + min(s[1], 4 - s[1])),
)
NS = len(SHIFTS)
QK_PARTS = 1
REDUCE_AT = (1, 5)
PREFIX_AT = (5, 8)
MESH = pl.DeviceIdType.MESH
C2 = 1.0 / (32.0**0.5)
BF = jnp.bfloat16
F32 = jnp.float32


def dot(a, b):
    return jnp.dot(a, b, preferred_element_type=F32)


def iota(shape, dim):
    return lax.broadcasted_iota(jnp.int32, shape, dim)


def kernel(
    tok_hbm, wq_hbm, wk_hbm, wv_hbm, wo_hbm, out,
    tok, wqk, wv, wo, q_s, k_s, kt, ktb, v_s, phiq, pk, ea, eb, lext, numer,
    sbuf, rbuf, xs, xbuf, obuf, pbuf, pre, att, sib, acc,
    tok_sem, wqk_sem, wv_sem, wo_sem,
    s_send, s_recv, x_send, x_recv, p_send, p_recv, a_send, a_recv,
):
    seq = lax.axis_index("seq")
    core = lax.axis_index("head")
    xp = seq // PLANE
    me = lax.rem(seq, PLANE)

    def wqk_copy(j):
        src = (wq_hbm, wk_hbm)[j]
        return pltpu.make_async_copy(src, wqk.at[:, pl.ds(j * 128, 128)], wqk_sem.at[j])

    def tok_copy(b):
        rows = pl.ds(b * CHUNK, CHUNK)
        return pltpu.make_async_copy(tok_hbm.at[rows, :], tok.at[rows, :], tok_sem.at[b])

    def wv_copy(j):
        cols = pl.ds(j * 512, 512)
        return pltpu.make_async_copy(wv_hbm.at[:, cols], wv.at[j], wv_sem.at[j])

    def wo_copy(j):
        side, half = j // 2, j % 2
        base = (core if side == 0 else 1 - core) * 1024 + half * 512
        rows = pl.ds(pl.multiple_of(base, 512), 512)
        cols = pl.ds(pl.multiple_of(core * 1024, 1024), 1024)
        return pltpu.make_async_copy(wo_hbm.at[rows, cols], wo.at[j], wo_sem.at[j])

    for j in range(2):
        wqk_copy(j).start()
    for b in range(NCH):
        tok_copy(b).start()

    barrier = pltpu.get_barrier_semaphore()

    def chip(i, sign=1):
        dy, dz = SHIFTS[i]
        y = lax.rem(me // 4 + 4 + sign * dy, 4)
        z = lax.rem(lax.rem(me, 4) + 4 + sign * dz, 4)
        return y * 4 + z

    for i in range(NS):
        pl.semaphore_signal(
            barrier, inc=1, device_id={"seq": xp * PLANE + chip(i)}, device_id_type=MESH
        )
    for dx in range(1, XN):
        pl.semaphore_signal(
            barrier,
            inc=1,
            device_id={"seq": lax.rem(xp + dx, XN) * PLANE + me},
            device_id_type=MESH,
        )
    pl.semaphore_signal(barrier, inc=1, device_id={"head": 1 - core}, device_id_type=MESH)

    row = iota((256, 256), 0)
    col = iota((256, 256), 1)
    lane_i = col & 15
    lane_d = (col >> 4) - 1
    ea[...] = jnp.where((row == 128 + lane_i) & (col < 152), 1.0, 0.0).astype(BF)
    eb[...] = jnp.where(
        (row == 128 + ((lane_i + lane_d) & 15)) & (col >= 16) & (col < 152), 1.0, 0.0
    ).astype(BF)

    for j in range(2):
        wqk_copy(j).wait()
    for part in range(QK_PARTS):
        each = NCH // QK_PARTS
        for b in range(part * each, part * each + each):
            tok_copy(b).wait()
        if part == 0:
            for j in range(2):
                wv_copy(j).start()
        rows = slice(part * each * CHUNK, (part + 1) * each * CHUNK)
        qk = dot(tok[rows, :], wqk[...])
        q_s[rows, :] = qk[:, :128].astype(BF)
        k_s[rows, :] = qk[:, 128:].astype(BF)
    for j in range(4):
        wo_copy(j).start()


    eye = iota((128, 128), 0) == iota((128, 128), 1)
    ones = jnp.ones((CHUNK, 128), BF)
    row_p = iota((PIECE, 128), 0)
    row16w = iota((16, TOK), 0)

    def state_copy(g, i):
        to = chip(i)
        return pltpu.make_async_remote_copy(
            src_ref=sbuf.at[g * PLANE + to], dst_ref=rbuf.at[g, me], send_sem=s_send.at[g, i],
            recv_sem=s_recv.at[g, i], device_id={"seq": xp * PLANE + to}, device_id_type=MESH,
        )

    def state_arrival(g, i):
        come = chip(i, -1)
        return pltpu.make_async_remote_copy(
            src_ref=sbuf.at[g * PLANE + come], dst_ref=rbuf.at[g, come], send_sem=s_send.at[g, i],
            recv_sem=s_recv.at[g, i], device_id={"seq": xp * PLANE + come}, device_id_type=MESH,
        )

    def total_copy(g, dx):
        return pltpu.make_async_remote_copy(
            src_ref=xs.at[g], dst_ref=xbuf.at[g, xp], send_sem=x_send.at[g, dx - 1],
            recv_sem=x_recv.at[g, dx - 1],
            device_id={"seq": lax.rem(xp + dx, XN) * PLANE + me}, device_id_type=MESH,
        )

    def total_arrival(g, dx):
        other = lax.rem(xp + XN - dx, XN)
        return pltpu.make_async_remote_copy(
            src_ref=xs.at[g], dst_ref=xbuf.at[g, other], send_sem=x_send.at[g, dx - 1],
            recv_sem=x_recv.at[g, dx - 1],
            device_id={"seq": other * PLANE + me}, device_id_type=MESH,
        )

    def prefix_copy(g, i):
        to = chip(i)
        return pltpu.make_async_remote_copy(
            src_ref=obuf.at[g, to], dst_ref=pbuf.at[g * PLANE + me], send_sem=p_send.at[g, i],
            recv_sem=p_recv.at[g, i], device_id={"seq": xp * PLANE + to}, device_id_type=MESH,
        )

    def prefix_arrival(g, i):
        come = chip(i, -1)
        return pltpu.make_async_remote_copy(
            src_ref=obuf.at[g, come], dst_ref=pbuf.at[g * PLANE + come], send_sem=p_send.at[g, i],
            recv_sem=p_recv.at[g, i], device_id={"seq": xp * PLANE + come}, device_id_type=MESH,
        )

    def att_copy(h):
        cols = pl.ds(h * 128, 128)
        return pltpu.make_async_remote_copy(
            src_ref=att.at[:, cols], dst_ref=sib.at[:, cols], send_sem=a_send.at[h],
            recv_sem=a_recv.at[h], device_id={"head": 1 - core}, device_id_type=MESH,
        )

    def values(g):
        wv_copy(g).wait()
        if g == 0:
            for b in range(NCH):
                rows = slice(b * CHUNK, (b + 1) * CHUNK)
                k_t = k_s[rows, :].T
                kt[:, rows] = k_t.astype(F32)
                ktb[:, rows] = k_t
        v_s[g] = dot(tok[...], wv[g]).astype(BF)

    def key_features(g):
        for j in range(4):
            h = 4 * g + j
            u = kt[h * 16 : (h + 1) * 16, :]
            pk[j, 0:16, :] = (u * 0.5).astype(BF)
            for d in range(8):
                other = u if d == 0 else pltpu.roll(u, 16 - d, 0)
                pk[j, 16 + 16 * d : 32 + 16 * d, :] = (u * other * C2).astype(BF)
            last = u * pltpu.roll(u, 8, 0) * C2
            last = jnp.where(row16w < 8, last, jnp.where(row16w == 8, 1.0, 0.0))
            pk[j, 144:160, :] = last.astype(BF)

    def states(g):
        for j in range(4):
            h = 4 * g + j
            run = None
            for b in range(NCH):
                rows = slice(b * CHUNK, (b + 1) * CHUNK)
                vals = jnp.concatenate([v_s[g, rows, j * 128 : (j + 1) * 128], ones], axis=1)
                part = dot(pk[j, :, rows], vals)
                run = part if run is None else run + part
                if b < NCH - 1:
                    lext[h, b] = run.astype(BF)
            zc = run[:, 128:]
            z0 = jnp.sum(jnp.where(eye, zc[:128], 0.0), axis=0, keepdims=True)
            z1 = jnp.sum(jnp.where(eye[:32], zc[128:], 0.0), axis=0, keepdims=True)
            for k in range(4):
                piece = run[k * PIECE : (k + 1) * PIECE, :128]
                if k == 3:
                    piece = jnp.where(row_p == 38, z0, jnp.where(row_p == 39, z1, piece))
                sbuf[h * 4 + k] = piece.astype(BF)

    def send_states(g):
        for i in range(NS):
            state_copy(g, i).start()
        rbuf[g, me] = sbuf[g * PLANE + me]

    lane = iota((1, 256), 1)
    c1 = jnp.where(lane < 16, 1.0, 0.0)
    c0 = jnp.where(lane == 152, 2.0, 0.0)
    scale = jnp.where(lane < 16, 1.0, jnp.where(lane < 32, 2.0 * C2, 4.0 * C2))
    lane128 = iota((1, 128), 1)
    causal = iota((CHUNK, CHUNK), 1) <= iota((CHUNK, CHUNK), 0)

    def inside(h):
        low = 128 - 16 * h
        ea_h = ea[low : low + 128, :]
        eb_h = eb[low : low + 128, :]
        own = jnp.where((lane128 >> 4) == h, 0.25, 0.0).astype(BF)
        vcols = slice((h % 4) * 128, (h % 4) * 128 + 128)
        for b in range(NCH):
            rows = slice(b * CHUNK, (b + 1) * CHUNK)
            qb = q_s[rows, :]
            first = dot(qb, ea_h)
            second = dot(qb, eb_h)
            feat = (first * (second + c1) * scale + c0).astype(BF)
            phiq[h, rows, :] = feat
            t = dot(qb * own, ktb[:, rows]) + 1.0
            t = jnp.where(causal, t * t + 1.0, 0.0).astype(BF)
            vals = jnp.concatenate([v_s[h // 4, rows, vcols], ones], axis=1)
            r = dot(t, vals)
            if b > 0:
                r = r + dot(feat[:, :FEAT], lext[h, b - 1])
            numer[h, rows, :] = r

    def reduce_step(g):
        for i in range(NS):
            state_arrival(g, i).wait_recv()
        tot = rbuf[g, 0].astype(F32)
        for q in range(1, PLANE):
            tot = tot + rbuf[g, q].astype(F32)
        xs[g] = tot.astype(BF)
        for dx in range(1, XN):
            pl.when(xp + dx < XN)(total_copy(g, dx).start)

    def prefix_step(g):
        for dx in range(1, XN):
            pl.when(xp >= dx)(total_arrival(g, dx).wait_recv)
        run = lax.fori_loop(
            0, xp, lambda k, a: a + xbuf[g, k].astype(F32), jnp.zeros((PIECE, 128), F32)
        )
        for q in range(PLANE):
            obuf[g, q] = run.astype(BF)
            run = run + rbuf[g, q].astype(F32)
        for i in range(NS):
            prefix_copy(g, i).start()
        pbuf[g * PLANE + me] = obuf[g, me]

    def slot(i):
        for g in range(2):
            if REDUCE_AT[g] == i:
                reduce_step(g)
            if PREFIX_AT[g] == i:
                prefix_step(g)

    ones128 = jnp.ones((128, 128), BF)

    def finish(g):
        for i in range(NS):
            prefix_arrival(g, i).wait_recv()
        for h in range(4 * g, 4 * g + 4):
            pieces = [pbuf[4 * h + k].astype(F32) for k in range(4)]
            z = pieces[3][38:40]
            m = jnp.concatenate(
                [jnp.where(eye, z[0:1], 0.0), jnp.where(eye[:32], z[1:2], 0.0)], axis=0
            )
            pre[h, :, :128] = jnp.concatenate(pieces, axis=0).astype(BF)
            pre[h, :, 128:] = dot(m.astype(BF), ones128).astype(BF)
        for h in range(4 * g, 4 * g + 4):
            for b in range(NCH):
                rows = slice(b * CHUNK, (b + 1) * CHUNK)
                r = dot(phiq[h, rows, :FEAT], pre[h]) + numer[h, rows, :]
                att[rows, h * 128 : (h + 1) * 128] = (r[:, :128] / r[:, 128:]).astype(BF)
            att_copy(h).start()

    def project(side, half, step):
        j = side * 2 + half
        wo_copy(j).wait()
        if side == 1:
            for h in range(4 * half, 4 * half + 4):
                att_copy(h).wait_recv()
        lhs = (att, sib)[side]
        for n in range(4):
            cols = slice(n * 256, (n + 1) * 256)
            r = dot(lhs[:, half * 512 : (half + 1) * 512], wo[j, :, cols])
            if step > 0:
                r = r + acc[:, cols]
            if step < 3:
                acc[:, cols] = r
            else:
                out[:, cols] = r.astype(BF)

    for g in range(2):
        values(g)
        key_features(g)
        states(g)
        if g == 0:
            pl.semaphore_wait(barrier, NS + XN - 1 + 1)
        send_states(g)
    slot(0)
    for h in range(HERE):
        inside(h)
        slot(h + 1)
    finish(0)
    project(0, 0, 0)
    project(1, 0, 1)
    finish(1)
    project(0, 1, 2)
    project(1, 1, 3)

    for g in range(2):
        for i in range(NS):
            state_copy(g, i).wait_send()
            prefix_copy(g, i).wait_send()
        for dx in range(1, XN):
            pl.when(xp + dx < XN)(total_copy(g, dx).wait_send)
    for h in range(HERE):
        att_copy(h).wait_send()


def per_device(tokens, w_query, w_key, w_value, w_out):
    vmem = pltpu.VMEM
    dma = pltpu.SemaphoreType.DMA
    hbm = pl.BlockSpec(memory_space=pl.ANY)
    return pl.pallas_call(
        kernel,
        out_shape=pltpu.VMEM((TOK, 1024), BF),
        in_specs=[hbm] * 5,
        out_specs=pl.BlockSpec(memory_space=pltpu.VMEM),
        scratch_shapes=[
            vmem((TOK, D), BF),
            vmem((D, 256), BF),
            vmem((2, D, 512), BF),
            vmem((4, 512, 1024), BF),
            vmem((TOK, 128), BF),
            vmem((TOK, 128), BF),
            vmem((128, TOK), F32),
            vmem((128, TOK), BF),
            vmem((2, TOK, 512), BF),
            vmem((HERE, TOK, 256), BF),
            vmem((4, FEAT, TOK), BF),
            vmem((256, 256), BF),
            vmem((256, 256), BF),
            vmem((HERE, NCH - 1, FEAT, 256), BF),
            vmem((HERE, TOK, 256), F32),
            vmem((2 * PLANE, PIECE, 128), BF),
            vmem((2, PLANE, PIECE, 128), BF),
            vmem((2, PIECE, 128), BF),
            vmem((2, XN, PIECE, 128), BF),
            vmem((2, PLANE, PIECE, 128), BF),
            vmem((2 * PLANE, PIECE, 128), BF),
            vmem((HERE, FEAT, 256), BF),
            vmem((TOK, 1024), BF),
            vmem((TOK, 1024), BF),
            vmem((TOK, 1024), F32),
            dma((NCH,)), dma((2,)), dma((2,)), dma((4,)),
            dma((2, NS)), dma((2, NS)), dma((2, XN - 1)), dma((2, XN - 1)),
            dma((2, NS)), dma((2, NS)), dma((HERE,)), dma((HERE,)),
        ],
        compiler_params=pltpu.CompilerParams(
            collective_id=0, has_side_effects=True, vmem_limit_bytes=56 * 1024 * 1024
        ),
    )(tokens, w_query, w_key, w_value, w_out)


def solution(mesh):
    in_specs = (P("seq", None), P(None, "head"), P(None, "head"), P(None, "head"), P())
    return jax.shard_map(
        per_device, mesh=mesh, in_specs=in_specs, out_specs=P("seq", "head"), check_vma=False
    )
```

```python
import jax
import jax.numpy as jnp
from jax import lax
from jax.experimental import pallas as pl
from jax.experimental.pallas import tpu as pltpu
from jax.sharding import PartitionSpec as P

TOK = 1024
D = 2048
HERE = 8
CHUNK = 256
NCH = TOK // CHUNK
FEAT = 160
PIECE = FEAT // 4
PLANE = 16
XN = 4
SHIFTS = sorted(
    [(dy, dz) for dy in range(4) for dz in range(4) if dy or dz],
    key=lambda s: -(min(s[0], 4 - s[0]) + min(s[1], 4 - s[1])),
)
NS = len(SHIFTS)
QK_PARTS = 1
REDUCE_AT = (1, 5)
PREFIX_AT = (5, 8)
MESH = pl.DeviceIdType.MESH
C2 = 1.0 / (32.0**0.5)
BF = jnp.bfloat16
F32 = jnp.float32


def dot(a, b):
    return jnp.dot(a, b, preferred_element_type=F32)


def iota(shape, dim):
    return lax.broadcasted_iota(jnp.int32, shape, dim)


def kernel(
    tok_hbm, wq_hbm, wk_hbm, wv_hbm, wo_hbm, out,
    tok, wqk, wv, wo, q_s, k_s, kt, ktb, v_s, phiq, pk, ea, eb, lext, numer,
    sbuf, rbuf, xs, xbuf, obuf, pbuf, pre, att, sib, acc,
    tok_sem, wqk_sem, wv_sem, wo_sem,
    s_send, s_recv, x_send, x_recv, p_send, p_recv, a_send, a_recv,
):
    seq = lax.axis_index("seq")
    core = lax.axis_index("head")
    xp = seq // PLANE
    me = lax.rem(seq, PLANE)

    def wqk_copy(j):
        src = (wq_hbm, wk_hbm)[j]
        return pltpu.make_async_copy(src, wqk.at[:, pl.ds(j * 128, 128)], wqk_sem.at[j])

    def tok_copy(b):
        rows = pl.ds(b * CHUNK, CHUNK)
        return pltpu.make_async_copy(tok_hbm.at[rows, :], tok.at[rows, :], tok_sem.at[b])

    def wv_copy(j):
        cols = pl.ds(j * 512, 512)
        return pltpu.make_async_copy(wv_hbm.at[:, cols], wv.at[j], wv_sem.at[j])

    def wo_copy(j):
        side, half = j // 2, j % 2
        base = (core if side == 0 else 1 - core) * 1024 + half * 512
        rows = pl.ds(pl.multiple_of(base, 512), 512)
        cols = pl.ds(pl.multiple_of(core * 1024, 1024), 1024)
        return pltpu.make_async_copy(wo_hbm.at[rows, cols], wo.at[j], wo_sem.at[j])

    for j in range(2):
        wqk_copy(j).start()
    for b in range(NCH):
        tok_copy(b).start()

    barrier = pltpu.get_barrier_semaphore()

    def chip(i, sign=1):
        dy, dz = SHIFTS[i]
        y = lax.rem(me // 4 + 4 + sign * dy, 4)
        z = lax.rem(lax.rem(me, 4) + 4 + sign * dz, 4)
        return y * 4 + z

    for i in range(NS):
        pl.semaphore_signal(
            barrier, inc=1, device_id={"seq": xp * PLANE + chip(i)}, device_id_type=MESH
        )
    for dx in range(1, XN):
        pl.semaphore_signal(
            barrier,
            inc=1,
            device_id={"seq": lax.rem(xp + dx, XN) * PLANE + me},
            device_id_type=MESH,
        )
    pl.semaphore_signal(barrier, inc=1, device_id={"head": 1 - core}, device_id_type=MESH)

    row = iota((256, 256), 0)
    col = iota((256, 256), 1)
    lane_i = col & 15
    lane_d = (col >> 4) - 1
    ea[...] = jnp.where((row == 128 + lane_i) & (col < 152), 1.0, 0.0).astype(BF)
    eb[...] = jnp.where(
        (row == 128 + ((lane_i + lane_d) & 15)) & (col >= 16) & (col < 152), 1.0, 0.0
    ).astype(BF)

    for j in range(2):
        wqk_copy(j).wait()
    for part in range(QK_PARTS):
        each = NCH // QK_PARTS
        for b in range(part * each, part * each + each):
            tok_copy(b).wait()
        if part == 0:
            for j in range(2):
                wv_copy(j).start()
        rows = slice(part * each * CHUNK, (part + 1) * each * CHUNK)
        qk = dot(tok[rows, :], wqk[...])
        q_s[rows, :] = qk[:, :128].astype(BF)
        k_s[rows, :] = qk[:, 128:].astype(BF)
    for j in range(4):
        wo_copy(j).start()


    eye = iota((128, 128), 0) == iota((128, 128), 1)
    ones = jnp.ones((CHUNK, 128), BF)
    row_p = iota((PIECE, 128), 0)
    row16w = iota((16, TOK), 0)

    def state_copy(g, i):
        to = chip(i)
        return pltpu.make_async_remote_copy(
            src_ref=sbuf.at[g * PLANE + to], dst_ref=rbuf.at[g, me], send_sem=s_send.at[g],
            recv_sem=s_recv.at[g], device_id={"seq": xp * PLANE + to}, device_id_type=MESH,
        )

    def all_states(g):
        return pltpu.make_async_remote_copy(
            src_ref=sbuf.at[pl.ds(g * PLANE, NS)], dst_ref=rbuf.at[g, pl.ds(0, NS)],
            send_sem=s_send.at[g], recv_sem=s_recv.at[g],
            device_id={"seq": xp * PLANE + chip(0)}, device_id_type=MESH,
        )

    def total_copy(g, dx):
        return pltpu.make_async_remote_copy(
            src_ref=xs.at[g], dst_ref=xbuf.at[g, xp], send_sem=x_send.at[g, dx - 1],
            recv_sem=x_recv.at[g, dx - 1],
            device_id={"seq": lax.rem(xp + dx, XN) * PLANE + me}, device_id_type=MESH,
        )

    def total_arrival(g, dx):
        other = lax.rem(xp + XN - dx, XN)
        return pltpu.make_async_remote_copy(
            src_ref=xs.at[g], dst_ref=xbuf.at[g, other], send_sem=x_send.at[g, dx - 1],
            recv_sem=x_recv.at[g, dx - 1],
            device_id={"seq": other * PLANE + me}, device_id_type=MESH,
        )

    def prefix_copy(g, i):
        to = chip(i)
        return pltpu.make_async_remote_copy(
            src_ref=obuf.at[g, to], dst_ref=pbuf.at[g * PLANE + me], send_sem=p_send.at[g],
            recv_sem=p_recv.at[g], device_id={"seq": xp * PLANE + to}, device_id_type=MESH,
        )

    def all_prefixes(g):
        return pltpu.make_async_remote_copy(
            src_ref=obuf.at[g, pl.ds(0, NS)], dst_ref=pbuf.at[pl.ds(g * PLANE, NS)],
            send_sem=p_send.at[g], recv_sem=p_recv.at[g],
            device_id={"seq": xp * PLANE + chip(0)}, device_id_type=MESH,
        )

    def att_copy(h):
        cols = pl.ds(h * 128, 128)
        return pltpu.make_async_remote_copy(
            src_ref=att.at[:, cols], dst_ref=sib.at[:, cols], send_sem=a_send.at[h // 4],
            recv_sem=a_recv.at[h // 4], device_id={"head": 1 - core}, device_id_type=MESH,
        )

    def all_att(half):
        cols = pl.ds(half * 512, 512)
        return pltpu.make_async_remote_copy(
            src_ref=att.at[:, cols], dst_ref=sib.at[:, cols], send_sem=a_send.at[half],
            recv_sem=a_recv.at[half], device_id={"head": 1 - core}, device_id_type=MESH,
        )

    def values(g):
        wv_copy(g).wait()
        if g == 0:
            for b in range(NCH):
                rows = slice(b * CHUNK, (b + 1) * CHUNK)
                k_t = k_s[rows, :].T
                kt[:, rows] = k_t.astype(F32)
                ktb[:, rows] = k_t
        v_s[g] = dot(tok[...], wv[g]).astype(BF)

    def key_features(g):
        for j in range(4):
            h = 4 * g + j
            u = kt[h * 16 : (h + 1) * 16, :]
            pk[j, 0:16, :] = (u * 0.5).astype(BF)
            for d in range(8):
                other = u if d == 0 else pltpu.roll(u, 16 - d, 0)
                pk[j, 16 + 16 * d : 32 + 16 * d, :] = (u * other * C2).astype(BF)
            last = u * pltpu.roll(u, 8, 0) * C2
            last = jnp.where(row16w < 8, last, jnp.where(row16w == 8, 1.0, 0.0))
            pk[j, 144:160, :] = last.astype(BF)

    def states(g):
        for j in range(4):
            h = 4 * g + j
            run = None
            for b in range(NCH):
                rows = slice(b * CHUNK, (b + 1) * CHUNK)
                vals = jnp.concatenate([v_s[g, rows, j * 128 : (j + 1) * 128], ones], axis=1)
                part = dot(pk[j, :, rows], vals)
                run = part if run is None else run + part
                if b < NCH - 1:
                    lext[h, b] = run.astype(BF)
            zc = run[:, 128:]
            z0 = jnp.sum(jnp.where(eye, zc[:128], 0.0), axis=0, keepdims=True)
            z1 = jnp.sum(jnp.where(eye[:32], zc[128:], 0.0), axis=0, keepdims=True)
            for k in range(4):
                piece = run[k * PIECE : (k + 1) * PIECE, :128]
                if k == 3:
                    piece = jnp.where(row_p == 38, z0, jnp.where(row_p == 39, z1, piece))
                sbuf[h * 4 + k] = piece.astype(BF)

    def send_states(g):
        for i in range(NS):
            state_copy(g, i).start()
        rbuf[g, me] = sbuf[g * PLANE + me]

    lane = iota((1, 256), 1)
    c1 = jnp.where(lane < 16, 1.0, 0.0)
    c0 = jnp.where(lane == 152, 2.0, 0.0)
    scale = jnp.where(lane < 16, 1.0, jnp.where(lane < 32, 2.0 * C2, 4.0 * C2))
    lane128 = iota((1, 128), 1)
    causal = iota((CHUNK, CHUNK), 1) <= iota((CHUNK, CHUNK), 0)

    def inside(h):
        low = 128 - 16 * h
        ea_h = ea[low : low + 128, :]
        eb_h = eb[low : low + 128, :]
        own = jnp.where((lane128 >> 4) == h, 0.25, 0.0).astype(BF)
        vcols = slice((h % 4) * 128, (h % 4) * 128 + 128)
        for b in range(NCH):
            rows = slice(b * CHUNK, (b + 1) * CHUNK)
            qb = q_s[rows, :]
            first = dot(qb, ea_h)
            second = dot(qb, eb_h)
            feat = (first * (second + c1) * scale + c0).astype(BF)
            phiq[h, rows, :] = feat
            t = dot(qb * own, ktb[:, rows]) + 1.0
            t = jnp.where(causal, t * t + 1.0, 0.0).astype(BF)
            vals = jnp.concatenate([v_s[h // 4, rows, vcols], ones], axis=1)
            r = dot(t, vals)
            if b > 0:
                r = r + dot(feat[:, :FEAT], lext[h, b - 1])
            numer[h, rows, :] = r

    def reduce_step(g):
        all_states(g).wait_recv()
        tot = rbuf[g, 0].astype(F32)
        for q in range(1, PLANE):
            tot = tot + rbuf[g, q].astype(F32)
        xs[g] = tot.astype(BF)
        for dx in range(1, XN):
            pl.when(xp + dx < XN)(total_copy(g, dx).start)

    def prefix_step(g):
        for dx in range(1, XN):
            pl.when(xp >= dx)(total_arrival(g, dx).wait_recv)
        run = lax.fori_loop(
            0, xp, lambda k, a: a + xbuf[g, k].astype(F32), jnp.zeros((PIECE, 128), F32)
        )
        for q in range(PLANE):
            obuf[g, q] = run.astype(BF)
            run = run + rbuf[g, q].astype(F32)
        for i in range(NS):
            prefix_copy(g, i).start()
        pbuf[g * PLANE + me] = obuf[g, me]

    def slot(i):
        for g in range(2):
            if REDUCE_AT[g] == i:
                reduce_step(g)
            if PREFIX_AT[g] == i:
                prefix_step(g)

    ones128 = jnp.ones((128, 128), BF)

    def finish(g):
        all_prefixes(g).wait_recv()
        for h in range(4 * g, 4 * g + 4):
            pieces = [pbuf[4 * h + k].astype(F32) for k in range(4)]
            z = pieces[3][38:40]
            m = jnp.concatenate(
                [jnp.where(eye, z[0:1], 0.0), jnp.where(eye[:32], z[1:2], 0.0)], axis=0
            )
            pre[h, :, :128] = jnp.concatenate(pieces, axis=0).astype(BF)
            pre[h, :, 128:] = dot(m.astype(BF), ones128).astype(BF)
        for h in range(4 * g, 4 * g + 4):
            for b in range(NCH):
                rows = slice(b * CHUNK, (b + 1) * CHUNK)
                r = dot(phiq[h, rows, :FEAT], pre[h]) + numer[h, rows, :]
                att[rows, h * 128 : (h + 1) * 128] = (r[:, :128] / r[:, 128:]).astype(BF)
            att_copy(h).start()

    def project(side, half, step):
        j = side * 2 + half
        wo_copy(j).wait()
        if side == 1:
            all_att(half).wait_recv()
        lhs = (att, sib)[side]
        for n in range(4):
            cols = slice(n * 256, (n + 1) * 256)
            r = dot(lhs[:, half * 512 : (half + 1) * 512], wo[j, :, cols])
            if step > 0:
                r = r + acc[:, cols]
            if step < 3:
                acc[:, cols] = r
            else:
                out[:, cols] = r.astype(BF)

    def drain():
        for g in range(2):
            all_states(g).wait_send()
            all_prefixes(g).wait_send()
            for dx in range(1, XN):
                pl.when(xp + dx < XN)(total_copy(g, dx).wait_send)
        for half in range(2):
            all_att(half).wait_send()

    for g in range(2):
        values(g)
        key_features(g)
        states(g)
        if g == 0:
            pl.semaphore_wait(barrier, NS + XN - 1 + 1)
        send_states(g)
    slot(0)
    for h in range(HERE):
        inside(h)
        slot(h + 1)
    finish(0)
    project(0, 0, 0)
    finish(1)
    project(0, 1, 1)
    project(1, 0, 2)
    project(1, 1, 3)
    drain()


def per_device(tokens, w_query, w_key, w_value, w_out):
    vmem = pltpu.VMEM
    dma = pltpu.SemaphoreType.DMA
    hbm = pl.BlockSpec(memory_space=pl.ANY)
    return pl.pallas_call(
        kernel,
        out_shape=pltpu.VMEM((TOK, 1024), BF),
        in_specs=[hbm] * 5,
        out_specs=pl.BlockSpec(memory_space=pltpu.VMEM),
        scratch_shapes=[
            vmem((TOK, D), BF),
            vmem((D, 256), BF),
            vmem((2, D, 512), BF),
            vmem((4, 512, 1024), BF),
            vmem((TOK, 128), BF),
            vmem((TOK, 128), BF),
            vmem((128, TOK), F32),
            vmem((128, TOK), BF),
            vmem((2, TOK, 512), BF),
            vmem((HERE, TOK, 256), BF),
            vmem((4, FEAT, TOK), BF),
            vmem((256, 256), BF),
            vmem((256, 256), BF),
            vmem((HERE, NCH - 1, FEAT, 256), BF),
            vmem((HERE, TOK, 256), F32),
            vmem((2 * PLANE, PIECE, 128), BF),
            vmem((2, PLANE, PIECE, 128), BF),
            vmem((2, PIECE, 128), BF),
            vmem((2, XN, PIECE, 128), BF),
            vmem((2, PLANE, PIECE, 128), BF),
            vmem((2 * PLANE, PIECE, 128), BF),
            vmem((HERE, FEAT, 256), BF),
            vmem((TOK, 1024), BF),
            vmem((TOK, 1024), BF),
            vmem((TOK, 1024), F32),
            dma((NCH,)), dma((2,)), dma((2,)), dma((4,)),
            dma((2,)), dma((2,)), dma((2, XN - 1)), dma((2, XN - 1)),
            dma((2,)), dma((2,)), dma((2,)), dma((2,)),
        ],
        compiler_params=pltpu.CompilerParams(
            collective_id=0, has_side_effects=True, vmem_limit_bytes=56 * 1024 * 1024
        ),
    )(tokens, w_query, w_key, w_value, w_out)


def solution(mesh):
    in_specs = (P("seq", None), P(None, "head"), P(None, "head"), P(None, "head"), P())
    return jax.shard_map(
        per_device, mesh=mesh, in_specs=in_specs, out_specs=P("seq", "head"), check_vma=False
    )
```

```python
import jax
import jax.numpy as jnp
from jax import lax
from jax.experimental import pallas as pl
from jax.experimental.pallas import tpu as pltpu
from jax.sharding import PartitionSpec as P

TOK = 1024
D = 2048
HERE = 8
CHUNK = 256
NCH = TOK // CHUNK
FEAT = 160
PIECE = FEAT // 4
PLANE = 16
XN = 4
SHIFTS = sorted(
    [(dy, dz) for dy in range(4) for dz in range(4) if dy or dz],
    key=lambda s: -(min(s[0], 4 - s[0]) + min(s[1], 4 - s[1])),
)
NS = len(SHIFTS)
QK_PARTS = 2
REDUCE_AT = (1, 5)
PREFIX_AT = (5, 8)
MESH = pl.DeviceIdType.MESH
C2 = 1.0 / (32.0**0.5)
BF = jnp.bfloat16
F32 = jnp.float32


def dot(a, b):
    return jnp.dot(a, b, preferred_element_type=F32)


def iota(shape, dim):
    return lax.broadcasted_iota(jnp.int32, shape, dim)


def kernel(
    tok_hbm, wq_hbm, wk_hbm, wv_hbm, wo_hbm, out,
    tok, wqk, wv, wo, q_s, k_s, kt, ktb, v_s, phiq, pk, pick, lext, t_s, numer,
    sbuf, rbuf, xs, xbuf, obuf, pbuf, pre, att, sib, acc,
    tok_sem, wqk_sem, wv_sem, wo_sem,
    s_send, s_recv, x_send, x_recv, p_send, p_recv, a_send, a_recv,
):
    seq = lax.axis_index("seq")
    core = lax.axis_index("head")
    xp = seq // PLANE
    me = lax.rem(seq, PLANE)

    def wqk_copy(j):
        src = (wq_hbm, wk_hbm)[j]
        return pltpu.make_async_copy(src, wqk.at[:, pl.ds(j * 128, 128)], wqk_sem.at[j])

    def tok_copy(b):
        rows = pl.ds(b * CHUNK, CHUNK)
        return pltpu.make_async_copy(tok_hbm.at[rows, :], tok.at[rows, :], tok_sem.at[b])

    def wv_copy(j):
        cols = pl.ds(j * 512, 512)
        return pltpu.make_async_copy(wv_hbm.at[:, cols], wv.at[j], wv_sem.at[j])

    def wo_copy(j):
        side, half = j // 2, j % 2
        base = (core if side == 0 else 1 - core) * 1024 + half * 512
        rows = pl.ds(pl.multiple_of(base, 512), 512)
        cols = pl.ds(pl.multiple_of(core * 1024, 1024), 1024)
        return pltpu.make_async_copy(wo_hbm.at[rows, cols], wo.at[j], wo_sem.at[j])

    for j in range(2):
        wqk_copy(j).start()
    for b in range(NCH):
        tok_copy(b).start()
    wv_copy(0).start()

    barrier = pltpu.get_barrier_semaphore()

    def chip(i, sign=1):
        dy, dz = SHIFTS[i]
        y = lax.rem(me // 4 + 4 + sign * dy, 4)
        z = lax.rem(lax.rem(me, 4) + 4 + sign * dz, 4)
        return y * 4 + z

    for i in range(NS):
        pl.semaphore_signal(
            barrier, inc=1, device_id={"seq": xp * PLANE + chip(i)}, device_id_type=MESH
        )
    for dx in range(1, XN):
        pl.semaphore_signal(
            barrier,
            inc=1,
            device_id={"seq": lax.rem(xp + dx, XN) * PLANE + me},
            device_id_type=MESH,
        )
    pl.semaphore_signal(barrier, inc=1, device_id={"head": 1 - core}, device_id_type=MESH)

    row = iota((256, 256), 0)
    col = iota((256, 256), 1)
    shift = jnp.where(col < 128, 0, (col - 128) >> 4)
    pick[...] = jnp.where(row == 128 + (((col & 15) + shift) & 15), 1.0, 0.0).astype(BF)

    for j in range(2):
        wqk_copy(j).wait()
    for b in range(NCH):
        tok_copy(b).wait()
    wv_copy(1).start()
    for part in range(QK_PARTS):
        each = TOK // QK_PARTS
        rows = slice(part * each, (part + 1) * each)
        qk = dot(tok[rows, :], wqk[...])
        q_s[rows, :] = qk[:, :128].astype(BF)
        k_s[rows, :] = qk[:, 128:].astype(BF)
    for j in range(4):
        wo_copy(j).start()


    eye = iota((128, 128), 0) == iota((128, 128), 1)
    ones = jnp.ones((CHUNK, 128), BF)
    row_p = iota((PIECE, 128), 0)
    row16w = iota((16, TOK), 0)

    def state_copy(g, i):
        to = chip(i)
        return pltpu.make_async_remote_copy(
            src_ref=sbuf.at[g * PLANE + to], dst_ref=rbuf.at[g, me], send_sem=s_send.at[g],
            recv_sem=s_recv.at[g], device_id={"seq": xp * PLANE + to}, device_id_type=MESH,
        )

    def all_states(g):
        return pltpu.make_async_remote_copy(
            src_ref=sbuf.at[pl.ds(g * PLANE, NS)], dst_ref=rbuf.at[g, pl.ds(0, NS)],
            send_sem=s_send.at[g], recv_sem=s_recv.at[g],
            device_id={"seq": xp * PLANE + chip(0)}, device_id_type=MESH,
        )

    def total_copy(g, dx):
        return pltpu.make_async_remote_copy(
            src_ref=xs.at[g], dst_ref=xbuf.at[g, xp], send_sem=x_send.at[g, dx - 1],
            recv_sem=x_recv.at[g, dx - 1],
            device_id={"seq": lax.rem(xp + dx, XN) * PLANE + me}, device_id_type=MESH,
        )

    def total_arrival(g, dx):
        other = lax.rem(xp + XN - dx, XN)
        return pltpu.make_async_remote_copy(
            src_ref=xs.at[g], dst_ref=xbuf.at[g, other], send_sem=x_send.at[g, dx - 1],
            recv_sem=x_recv.at[g, dx - 1],
            device_id={"seq": other * PLANE + me}, device_id_type=MESH,
        )

    def prefix_copy(g, i):
        to = chip(i)
        return pltpu.make_async_remote_copy(
            src_ref=obuf.at[g, to], dst_ref=pbuf.at[g * PLANE + me], send_sem=p_send.at[g],
            recv_sem=p_recv.at[g], device_id={"seq": xp * PLANE + to}, device_id_type=MESH,
        )

    def all_prefixes(g):
        return pltpu.make_async_remote_copy(
            src_ref=obuf.at[g, pl.ds(0, NS)], dst_ref=pbuf.at[pl.ds(g * PLANE, NS)],
            send_sem=p_send.at[g], recv_sem=p_recv.at[g],
            device_id={"seq": xp * PLANE + chip(0)}, device_id_type=MESH,
        )

    def att_copy(h):
        cols = pl.ds(h * 128, 128)
        return pltpu.make_async_remote_copy(
            src_ref=att.at[:, cols], dst_ref=sib.at[:, cols], send_sem=a_send.at[h // 4],
            recv_sem=a_recv.at[h // 4], device_id={"head": 1 - core}, device_id_type=MESH,
        )

    def all_att(half):
        cols = pl.ds(half * 512, 512)
        return pltpu.make_async_remote_copy(
            src_ref=att.at[:, cols], dst_ref=sib.at[:, cols], send_sem=a_send.at[half],
            recv_sem=a_recv.at[half], device_id={"head": 1 - core}, device_id_type=MESH,
        )

    def values(g):
        wv_copy(g).wait()
        if g == 0:
            for b in range(NCH):
                rows = slice(b * CHUNK, (b + 1) * CHUNK)
                k_t = k_s[rows, :].T
                kt[:, rows] = k_t.astype(F32)
                ktb[:, rows] = k_t
        v_s[g] = dot(tok[...], wv[g]).astype(BF)

    def key_features(g):
        for j in range(4):
            h = 4 * g + j
            u = kt[h * 16 : (h + 1) * 16, :]
            pk[j, 128:144, :] = (u * 0.5).astype(BF)
            for d in range(8):
                other = u if d == 0 else pltpu.roll(u, 16 - d, 0)
                pk[j, 16 * d : 16 * d + 16, :] = (u * other * C2).astype(BF)
            last = u * pltpu.roll(u, 8, 0) * C2
            last = jnp.where(row16w < 8, last, jnp.where(row16w == 8, 1.0, 0.0))
            pk[j, 144:160, :] = last.astype(BF)

    def states(g):
        for j in range(4):
            h = 4 * g + j
            run = None
            for b in range(NCH):
                rows = slice(b * CHUNK, (b + 1) * CHUNK)
                vals = jnp.concatenate([v_s[g, rows, j * 128 : (j + 1) * 128], ones], axis=1)
                part = dot(pk[j, :, rows], vals)
                run = part if run is None else run + part
                if b < NCH - 1:
                    lext[h, b] = run.astype(BF)
            zc = run[:, 128:]
            z0 = jnp.sum(jnp.where(eye, zc[:128], 0.0), axis=0, keepdims=True)
            z1 = jnp.sum(jnp.where(eye[:32], zc[128:], 0.0), axis=0, keepdims=True)
            for k in range(4):
                piece = run[k * PIECE : (k + 1) * PIECE, :128]
                if k == 3:
                    piece = jnp.where(row_p == 38, z0, jnp.where(row_p == 39, z1, piece))
                sbuf[h * 4 + k] = piece.astype(BF)

    def send_states(g):
        for i in range(NS):
            state_copy(g, i).start()
        rbuf[g, me] = sbuf[g * PLANE + me]

    lane128 = iota((1, 128), 1)
    scale = jnp.where(lane128 < 16, 2.0 * C2, 4.0 * C2)
    const = jnp.where(lane128 == 24, 2.0, 0.0)
    causal = iota((CHUNK, CHUNK), 1) <= iota((CHUNK, CHUNK), 0)

    def weights(h, b):
        rows = slice(b * CHUNK, (b + 1) * CHUNK)
        low = 128 - 16 * h
        qb = q_s[rows, :]
        both = dot(qb, pick[low : low + 128, :])
        own = jnp.where((lane128 >> 4) == h, 0.25, 0.0).astype(BF)
        t = dot(qb * own, ktb[:, rows]) + 1.0
        one = both[:, :128]
        far = one * pltpu.roll(one, 8, 1) * (4.0 * C2)
        last = jnp.where(lane128 < 16, one, jnp.where(lane128 < 24, far, const))
        feat = jnp.concatenate([one * both[:, 128:] * scale, last], axis=1).astype(BF)
        phiq[h, rows, :] = feat
        t_s[h % 2, b] = jnp.where(causal, t * t + 1.0, 0.0).astype(BF)

    def collect(h, b):
        rows = slice(b * CHUNK, (b + 1) * CHUNK)
        vcols = slice((h % 4) * 128, (h % 4) * 128 + 128)
        vals = jnp.concatenate([v_s[h // 4, rows, vcols], ones], axis=1)
        r = dot(t_s[h % 2, b], vals)
        if b > 0:
            r = r + dot(phiq[h, rows, :FEAT], lext[h, b - 1])
        numer[h, rows, :] = r

    def inside(h):
        for b in range(NCH):
            if h + 1 < HERE:
                weights(h + 1, b)
            collect(h, b)

    def reduce_step(g):
        all_states(g).wait_recv()
        tot = rbuf[g, 0].astype(F32)
        for q in range(1, PLANE):
            tot = tot + rbuf[g, q].astype(F32)
        xs[g] = tot.astype(BF)
        for dx in range(1, XN):
            pl.when(xp + dx < XN)(total_copy(g, dx).start)

    def prefix_step(g):
        for dx in range(1, XN):
            pl.when(xp >= dx)(total_arrival(g, dx).wait_recv)
        run = lax.fori_loop(
            0, xp, lambda k, a: a + xbuf[g, k].astype(F32), jnp.zeros((PIECE, 128), F32)
        )
        for q in range(PLANE):
            obuf[g, q] = run.astype(BF)
            run = run + rbuf[g, q].astype(F32)
        for i in range(NS):
            prefix_copy(g, i).start()
        pbuf[g * PLANE + me] = obuf[g, me]

    def slot(i):
        for g in range(2):
            if REDUCE_AT[g] == i:
                reduce_step(g)
            if PREFIX_AT[g] == i:
                prefix_step(g)

    ones128 = jnp.ones((128, 128), BF)

    def finish(g):
        all_prefixes(g).wait_recv()
        for h in range(4 * g, 4 * g + 4):
            pieces = [pbuf[4 * h + k].astype(F32) for k in range(4)]
            z = pieces[3][38:40]
            m = jnp.concatenate(
                [jnp.where(eye, z[0:1], 0.0), jnp.where(eye[:32], z[1:2], 0.0)], axis=0
            )
            pre[h, :, :128] = jnp.concatenate(pieces, axis=0).astype(BF)
            pre[h, :, 128:] = dot(m.astype(BF), ones128).astype(BF)
        for h in range(4 * g, 4 * g + 4):
            for b in range(NCH):
                rows = slice(b * CHUNK, (b + 1) * CHUNK)
                r = dot(phiq[h, rows, :FEAT], pre[h]) + numer[h, rows, :]
                att[rows, h * 128 : (h + 1) * 128] = (r[:, :128] / r[:, 128:]).astype(BF)
            att_copy(h).start()

    def project(side, half, step):
        j = side * 2 + half
        wo_copy(j).wait()
        if side == 1:
            all_att(half).wait_recv()
        lhs = (att, sib)[side]
        for n in range(4):
            cols = slice(n * 256, (n + 1) * 256)
            r = dot(lhs[:, half * 512 : (half + 1) * 512], wo[j, :, cols])
            if step > 0:
                r = r + acc[:, cols]
            if step < 3:
                acc[:, cols] = r
            else:
                out[:, cols] = r.astype(BF)

    def drain():
        for g in range(2):
            all_states(g).wait_send()
            all_prefixes(g).wait_send()
            for dx in range(1, XN):
                pl.when(xp + dx < XN)(total_copy(g, dx).wait_send)
        for half in range(2):
            all_att(half).wait_send()

    for g in range(2):
        values(g)
        key_features(g)
        states(g)
        if g == 0:
            pl.semaphore_wait(barrier, NS + XN - 1 + 1)
        send_states(g)
    slot(0)
    for b in range(NCH):
        weights(0, b)
    for h in range(HERE):
        inside(h)
        slot(h + 1)
    finish(0)
    project(0, 0, 0)
    finish(1)
    project(0, 1, 1)
    project(1, 0, 2)
    project(1, 1, 3)
    drain()


def per_device(tokens, w_query, w_key, w_value, w_out):
    vmem = pltpu.VMEM
    dma = pltpu.SemaphoreType.DMA
    hbm = pl.BlockSpec(memory_space=pl.ANY)
    return pl.pallas_call(
        kernel,
        out_shape=pltpu.VMEM((TOK, 1024), BF),
        in_specs=[hbm] * 5,
        out_specs=pl.BlockSpec(memory_space=pltpu.VMEM),
        scratch_shapes=[
            vmem((TOK, D), BF),
            vmem((D, 256), BF),
            vmem((2, D, 512), BF),
            vmem((4, 512, 1024), BF),
            vmem((TOK, 128), BF),
            vmem((TOK, 128), BF),
            vmem((128, TOK), F32),
            vmem((128, TOK), BF),
            vmem((2, TOK, 512), BF),
            vmem((HERE, TOK, 256), BF),
            vmem((4, FEAT, TOK), BF),
            vmem((256, 256), BF),
            vmem((HERE, NCH - 1, FEAT, 256), BF),
            vmem((2, NCH, CHUNK, CHUNK), BF),
            vmem((HERE, TOK, 256), F32),
            vmem((2 * PLANE, PIECE, 128), BF),
            vmem((2, PLANE, PIECE, 128), BF),
            vmem((2, PIECE, 128), BF),
            vmem((2, XN, PIECE, 128), BF),
            vmem((2, PLANE, PIECE, 128), BF),
            vmem((2 * PLANE, PIECE, 128), BF),
            vmem((HERE, FEAT, 256), BF),
            vmem((TOK, 1024), BF),
            vmem((TOK, 1024), BF),
            vmem((TOK, 1024), F32),
            dma((NCH,)), dma((2,)), dma((2,)), dma((4,)),
            dma((2,)), dma((2,)), dma((2, XN - 1)), dma((2, XN - 1)),
            dma((2,)), dma((2,)), dma((2,)), dma((2,)),
        ],
        compiler_params=pltpu.CompilerParams(
            collective_id=0, has_side_effects=True, vmem_limit_bytes=56 * 1024 * 1024
        ),
    )(tokens, w_query, w_key, w_value, w_out)


def solution(mesh):
    in_specs = (P("seq", None), P(None, "head"), P(None, "head"), P(None, "head"), P())
    return jax.shard_map(
        per_device, mesh=mesh, in_specs=in_specs, out_specs=P("seq", "head"), check_vma=False
    )
```

```python
import jax
import jax.numpy as jnp
from jax import lax
from jax.experimental import pallas as pl
from jax.experimental.pallas import tpu as pltpu
from jax.sharding import PartitionSpec as P

TOK = 1024
D = 2048
HERE = 8
CHUNK = 256
NCH = TOK // CHUNK
FEAT = 160
PIECE = FEAT // 4
PLANE = 16
XN = 4
SHIFTS = sorted(
    [(dy, dz) for dy in range(4) for dz in range(4) if dy or dz],
    key=lambda s: -(min(s[0], 4 - s[0]) + min(s[1], 4 - s[1])),
)
NS = len(SHIFTS)
QK_PARTS = 2
REDUCE_AT = (1, 5)
PREFIX_AT = (5, 7)
MESH = pl.DeviceIdType.MESH
C2 = 1.0 / (32.0**0.5)
BF = jnp.bfloat16
F32 = jnp.float32


def dot(a, b):
    return jnp.dot(a, b, preferred_element_type=F32)


def iota(shape, dim):
    return lax.broadcasted_iota(jnp.int32, shape, dim)


def kernel(
    tok_hbm, wq_hbm, wk_hbm, wv_hbm, wo_hbm, out,
    tok, wqk, wv, wo, q_s, k_s, kt, ktb, v_s, phiq, pk, pick, lext, t_s, numer,
    sbuf, rbuf, xs, xbuf, obuf, pbuf, pre, att, sib, acc,
    tok_sem, wqk_sem, wv_sem, wo_sem,
    s_send, s_recv, x_send, x_recv, p_send, p_recv, a_send, a_recv,
):
    seq = lax.axis_index("seq")
    core = lax.axis_index("head")
    xp = seq // PLANE
    me = lax.rem(seq, PLANE)

    def wqk_copy(j):
        src = (wq_hbm, wk_hbm)[j]
        return pltpu.make_async_copy(src, wqk.at[:, pl.ds(j * 128, 128)], wqk_sem.at[j])

    def tok_copy(b):
        rows = pl.ds(b * CHUNK, CHUNK)
        return pltpu.make_async_copy(tok_hbm.at[rows, :], tok.at[rows, :], tok_sem.at[b])

    def wv_copy(j):
        cols = pl.ds(j * 512, 512)
        return pltpu.make_async_copy(wv_hbm.at[:, cols], wv.at[j], wv_sem.at[j])

    def wo_copy(j):
        side, half = j // 2, j % 2
        base = (core if side == 0 else 1 - core) * 1024 + half * 512
        rows = pl.ds(pl.multiple_of(base, 512), 512)
        cols = pl.ds(pl.multiple_of(core * 1024, 1024), 1024)
        return pltpu.make_async_copy(wo_hbm.at[rows, cols], wo.at[j], wo_sem.at[j])

    for j in range(2):
        wqk_copy(j).start()
    for b in range(NCH):
        tok_copy(b).start()
    wv_copy(0).start()

    barrier = pltpu.get_barrier_semaphore()

    def chip(i, sign=1):
        dy, dz = SHIFTS[i]
        y = lax.rem(me // 4 + 4 + sign * dy, 4)
        z = lax.rem(lax.rem(me, 4) + 4 + sign * dz, 4)
        return y * 4 + z

    for i in range(NS):
        pl.semaphore_signal(
            barrier, inc=1, device_id={"seq": xp * PLANE + chip(i)}, device_id_type=MESH
        )
    for dx in range(1, XN):
        pl.semaphore_signal(
            barrier,
            inc=1,
            device_id={"seq": lax.rem(xp + dx, XN) * PLANE + me},
            device_id_type=MESH,
        )
    pl.semaphore_signal(barrier, inc=1, device_id={"head": 1 - core}, device_id_type=MESH)

    row = iota((256, 256), 0)
    col = iota((256, 256), 1)
    shift = jnp.where(col < 128, 0, (col - 128) >> 4)
    pick[...] = jnp.where(row == 128 + (((col & 15) + shift) & 15), 1.0, 0.0).astype(BF)

    for j in range(2):
        wqk_copy(j).wait()
    for b in range(NCH):
        tok_copy(b).wait()
    wv_copy(1).start()
    for part in range(QK_PARTS):
        each = TOK // QK_PARTS
        rows = slice(part * each, (part + 1) * each)
        qk = dot(tok[rows, :], wqk[...])
        q_s[rows, :] = qk[:, :128].astype(BF)
        k_s[rows, :] = qk[:, 128:].astype(BF)
    for j in range(4):
        wo_copy(j).start()


    eye = iota((128, 128), 0) == iota((128, 128), 1)
    ones = jnp.ones((CHUNK, 128), BF)
    row_p = iota((PIECE, 128), 0)
    row16w = iota((16, TOK), 0)

    def state_copy(g, i):
        to = chip(i)
        return pltpu.make_async_remote_copy(
            src_ref=sbuf.at[g * PLANE + to], dst_ref=rbuf.at[g, me], send_sem=s_send.at[g],
            recv_sem=s_recv.at[g], device_id={"seq": xp * PLANE + to}, device_id_type=MESH,
        )

    def all_states(g):
        return pltpu.make_async_remote_copy(
            src_ref=sbuf.at[pl.ds(g * PLANE, NS)], dst_ref=rbuf.at[g, pl.ds(0, NS)],
            send_sem=s_send.at[g], recv_sem=s_recv.at[g],
            device_id={"seq": xp * PLANE + chip(0)}, device_id_type=MESH,
        )

    def total_copy(g, dx):
        return pltpu.make_async_remote_copy(
            src_ref=xs.at[g], dst_ref=xbuf.at[g, xp], send_sem=x_send.at[g, dx - 1],
            recv_sem=x_recv.at[g, dx - 1],
            device_id={"seq": lax.rem(xp + dx, XN) * PLANE + me}, device_id_type=MESH,
        )

    def total_arrival(g, dx):
        other = lax.rem(xp + XN - dx, XN)
        return pltpu.make_async_remote_copy(
            src_ref=xs.at[g], dst_ref=xbuf.at[g, other], send_sem=x_send.at[g, dx - 1],
            recv_sem=x_recv.at[g, dx - 1],
            device_id={"seq": other * PLANE + me}, device_id_type=MESH,
        )

    def prefix_copy(g, i):
        to = chip(i)
        return pltpu.make_async_remote_copy(
            src_ref=obuf.at[g, to], dst_ref=pbuf.at[g * PLANE + me], send_sem=p_send.at[g],
            recv_sem=p_recv.at[g], device_id={"seq": xp * PLANE + to}, device_id_type=MESH,
        )

    def all_prefixes(g):
        return pltpu.make_async_remote_copy(
            src_ref=obuf.at[g, pl.ds(0, NS)], dst_ref=pbuf.at[pl.ds(g * PLANE, NS)],
            send_sem=p_send.at[g], recv_sem=p_recv.at[g],
            device_id={"seq": xp * PLANE + chip(0)}, device_id_type=MESH,
        )

    def att_copy(h):
        cols = pl.ds(h * 128, 128)
        return pltpu.make_async_remote_copy(
            src_ref=att.at[:, cols], dst_ref=sib.at[:, cols], send_sem=a_send.at[h // 4],
            recv_sem=a_recv.at[h // 4], device_id={"head": 1 - core}, device_id_type=MESH,
        )

    def all_att(half):
        cols = pl.ds(half * 512, 512)
        return pltpu.make_async_remote_copy(
            src_ref=att.at[:, cols], dst_ref=sib.at[:, cols], send_sem=a_send.at[half],
            recv_sem=a_recv.at[half], device_id={"head": 1 - core}, device_id_type=MESH,
        )

    def values(g):
        wv_copy(g).wait()
        if g == 0:
            for b in range(NCH):
                rows = slice(b * CHUNK, (b + 1) * CHUNK)
                k_t = k_s[rows, :].T
                kt[:, rows] = k_t.astype(F32)
                ktb[:, rows] = k_t
        v_s[g] = dot(tok[...], wv[g]).astype(BF)

    def key_features(g):
        for j in range(4):
            h = 4 * g + j
            u = kt[h * 16 : (h + 1) * 16, :]
            pk[j, 128:144, :] = (u * 0.5).astype(BF)
            for d in range(8):
                other = u if d == 0 else pltpu.roll(u, 16 - d, 0)
                pk[j, 16 * d : 16 * d + 16, :] = (u * other * C2).astype(BF)
            last = u * pltpu.roll(u, 8, 0) * C2
            last = jnp.where(row16w < 8, last, jnp.where(row16w == 8, 1.0, 0.0))
            pk[j, 144:160, :] = last.astype(BF)

    def states(g):
        for j in range(4):
            h = 4 * g + j
            run = None
            for b in range(NCH):
                rows = slice(b * CHUNK, (b + 1) * CHUNK)
                vals = jnp.concatenate([v_s[g, rows, j * 128 : (j + 1) * 128], ones], axis=1)
                part = dot(pk[j, :, rows], vals)
                run = part if run is None else run + part
                if b < NCH - 1:
                    lext[h, b] = run.astype(BF)
            zc = run[:, 128:]
            z0 = jnp.sum(jnp.where(eye, zc[:128], 0.0), axis=0, keepdims=True)
            z1 = jnp.sum(jnp.where(eye[:32], zc[128:], 0.0), axis=0, keepdims=True)
            for k in range(4):
                piece = run[k * PIECE : (k + 1) * PIECE, :128]
                if k == 3:
                    piece = jnp.where(row_p == 38, z0, jnp.where(row_p == 39, z1, piece))
                sbuf[h * 4 + k] = piece.astype(BF)

    def send_states(g):
        for i in range(NS):
            state_copy(g, i).start()
        rbuf[g, me] = sbuf[g * PLANE + me]

    lane128 = iota((1, 128), 1)
    scale = jnp.where(lane128 < 16, 2.0 * C2, 4.0 * C2)
    const = jnp.where(lane128 == 24, 2.0, 0.0)
    causal = iota((CHUNK, CHUNK), 1) <= iota((CHUNK, CHUNK), 0)

    def weights(h, b):
        rows = slice(b * CHUNK, (b + 1) * CHUNK)
        low = 128 - 16 * h
        qb = q_s[rows, :]
        both = dot(qb, pick[low : low + 128, :])
        own = jnp.where((lane128 >> 4) == h, 0.25, 0.0).astype(BF)
        t = dot(qb * own, ktb[:, rows]) + 1.0
        one = both[:, :128]
        far = one * pltpu.roll(one, 8, 1) * (4.0 * C2)
        last = jnp.where(lane128 < 16, one, jnp.where(lane128 < 24, far, const))
        feat = jnp.concatenate([one * both[:, 128:] * scale, last], axis=1).astype(BF)
        phiq[h, rows, :] = feat
        t_s[h % 2, b] = jnp.where(causal, t * t + 1.0, 0.0).astype(BF)

    def collect(h, b):
        rows = slice(b * CHUNK, (b + 1) * CHUNK)
        vcols = slice((h % 4) * 128, (h % 4) * 128 + 128)
        vals = jnp.concatenate([v_s[h // 4, rows, vcols], ones], axis=1)
        r = dot(t_s[h % 2, b], vals)
        if b > 0:
            r = r + dot(phiq[h, rows, :FEAT], lext[h, b - 1])
        numer[h, rows, :] = r

    def inside(h):
        for b in range(NCH):
            if h + 1 < HERE:
                weights(h + 1, b)
            collect(h, b)

    def reduce_step(g):
        all_states(g).wait_recv()
        tot = rbuf[g, 0].astype(F32)
        for q in range(1, PLANE):
            tot = tot + rbuf[g, q].astype(F32)
        xs[g] = tot.astype(BF)
        for dx in range(1, XN):
            pl.when(xp + dx < XN)(total_copy(g, dx).start)

    def prefix_step(g):
        for dx in range(1, XN):
            pl.when(xp >= dx)(total_arrival(g, dx).wait_recv)
        run = lax.fori_loop(
            0, xp, lambda k, a: a + xbuf[g, k].astype(F32), jnp.zeros((PIECE, 128), F32)
        )
        for q in range(PLANE):
            obuf[g, q] = run.astype(BF)
            run = run + rbuf[g, q].astype(F32)
        for i in range(NS):
            prefix_copy(g, i).start()
        pbuf[g * PLANE + me] = obuf[g, me]

    def slot(i):
        for g in range(2):
            if REDUCE_AT[g] == i:
                reduce_step(g)
            if PREFIX_AT[g] == i:
                prefix_step(g)

    ones128 = jnp.ones((128, 128), BF)

    def finish(g):
        all_prefixes(g).wait_recv()
        for h in range(4 * g, 4 * g + 4):
            pieces = [pbuf[4 * h + k].astype(F32) for k in range(4)]
            z = pieces[3][38:40]
            m = jnp.concatenate(
                [jnp.where(eye, z[0:1], 0.0), jnp.where(eye[:32], z[1:2], 0.0)], axis=0
            )
            pre[h, :, :128] = jnp.concatenate(pieces, axis=0).astype(BF)
            pre[h, :, 128:] = dot(m.astype(BF), ones128).astype(BF)
        for h in range(4 * g, 4 * g + 4):
            for b in range(NCH):
                rows = slice(b * CHUNK, (b + 1) * CHUNK)
                r = dot(phiq[h, rows, :FEAT], pre[h]) + numer[h, rows, :]
                att[rows, h * 128 : (h + 1) * 128] = (r[:, :128] / r[:, 128:]).astype(BF)
            att_copy(h).start()

    def project(side, half, step):
        j = side * 2 + half
        wo_copy(j).wait()
        if side == 1:
            all_att(half).wait_recv()
        lhs = (att, sib)[side]
        for n in range(4):
            cols = slice(n * 256, (n + 1) * 256)
            r = dot(lhs[:, half * 512 : (half + 1) * 512], wo[j, :, cols])
            if step > 0:
                r = r + acc[:, cols]
            if step < 3:
                acc[:, cols] = r
            else:
                out[:, cols] = r.astype(BF)

    def drain():
        for g in range(2):
            all_states(g).wait_send()
            all_prefixes(g).wait_send()
            for dx in range(1, XN):
                pl.when(xp + dx < XN)(total_copy(g, dx).wait_send)
        for half in range(2):
            all_att(half).wait_send()

    for g in range(2):
        values(g)
        key_features(g)
        states(g)
        if g == 0:
            pl.semaphore_wait(barrier, NS + XN - 1 + 1)
        send_states(g)
    slot(0)
    for b in range(NCH):
        weights(0, b)
    for h in range(HERE):
        inside(h)
        slot(h + 1)
    finish(0)
    project(0, 0, 0)
    finish(1)
    project(0, 1, 1)
    project(1, 0, 2)
    project(1, 1, 3)
    drain()


def per_device(tokens, w_query, w_key, w_value, w_out):
    vmem = pltpu.VMEM
    dma = pltpu.SemaphoreType.DMA
    hbm = pl.BlockSpec(memory_space=pl.ANY)
    return pl.pallas_call(
        kernel,
        out_shape=pltpu.VMEM((TOK, 1024), BF),
        in_specs=[hbm] * 5,
        out_specs=pl.BlockSpec(memory_space=pltpu.VMEM),
        scratch_shapes=[
            vmem((TOK, D), BF),
            vmem((D, 256), BF),
            vmem((2, D, 512), BF),
            vmem((4, 512, 1024), BF),
            vmem((TOK, 128), BF),
            vmem((TOK, 128), BF),
            vmem((128, TOK), F32),
            vmem((128, TOK), BF),
            vmem((2, TOK, 512), BF),
            vmem((HERE, TOK, 256), BF),
            vmem((4, FEAT, TOK), BF),
            vmem((256, 256), BF),
            vmem((HERE, NCH - 1, FEAT, 256), BF),
            vmem((2, NCH, CHUNK, CHUNK), BF),
            vmem((HERE, TOK, 256), F32),
            vmem((2 * PLANE, PIECE, 128), BF),
            vmem((2, PLANE, PIECE, 128), BF),
            vmem((2, PIECE, 128), BF),
            vmem((2, XN, PIECE, 128), BF),
            vmem((2, PLANE, PIECE, 128), BF),
            vmem((2 * PLANE, PIECE, 128), BF),
            vmem((HERE, FEAT, 256), BF),
            vmem((TOK, 1024), BF),
            vmem((TOK, 1024), BF),
            vmem((TOK, 1024), F32),
            dma((NCH,)), dma((2,)), dma((2,)), dma((4,)),
            dma((2,)), dma((2,)), dma((2, XN - 1)), dma((2, XN - 1)),
            dma((2,)), dma((2,)), dma((2,)), dma((2,)),
        ],
        compiler_params=pltpu.CompilerParams(
            collective_id=0, has_side_effects=True, vmem_limit_bytes=56 * 1024 * 1024
        ),
    )(tokens, w_query, w_key, w_value, w_out)


def solution(mesh):
    in_specs = (P("seq", None), P(None, "head"), P(None, "head"), P(None, "head"), P())
    return jax.shard_map(
        per_device, mesh=mesh, in_specs=in_specs, out_specs=P("seq", "head"), check_vma=False
    )
```
